8 devices in a mesh: dp: 1 (over z), row: 2 (over y), co: 2 (over x), ci: 2 (over core).
Axes of the slice: x: 2, y: 2, z: 1, core: 2. Of those that a mesh axis runs over, the one named last changes fastest.
Arguments:
- x_in: bfloat16 [8192, 3072], P(('dp', 'row'), ('co', 'ci'))
- w_up: bfloat16 [3072, 8192], P('row', ('co', 'ci'))
- w_down: bfloat16 [8192, 3072], P('row', ('co', 'ci'))
Outputs:
- output: bfloat16 [8192, 3072], P(('dp', 'row'), ('co', 'ci'))
All inputs are finite; a program needn't handle non-finite values.
Results may differ from the reference program's by a relative error of at most 0.001.
Values are sent between devices in bfloat16 or wider.
A program may use at most 1 GiB of HBM per device.

```python
import jax
import jax.numpy as jnp
from jax import lax

TOK_DEV = 4096
D = 3072
F = 8192
ROW_GROUPS = 2


def setup_inputs(seed: int = 0, part: int = 0) -> dict:
    root_key = jax.random.key(seed)
    key_x = jax.random.fold_in(jax.random.fold_in(root_key, 1), part)
    key_up = jax.random.fold_in(root_key, 2)
    key_down = jax.random.fold_in(root_key, 3)
    x_in = jax.random.normal(key_x, (ROW_GROUPS * TOK_DEV, D), jnp.float32)
    w_up = jax.random.normal(key_up, (D, F), jnp.float32) * (D ** -0.5)
    w_down = jax.random.normal(key_down, (F, D), jnp.float32) * (F ** -0.5)
    return {"x_in": x_in.astype(jnp.bfloat16), "w_up": w_up.astype(jnp.bfloat16), "w_down": w_down.astype(jnp.bfloat16)}


def reference(x_in, w_up, w_down):
    x_blocks = x_in.reshape(ROW_GROUPS, TOK_DEV, D)

    def row_block(x_rows):
        pre_act = jnp.dot(x_rows, w_up, preferred_element_type=jnp.float32)
        hidden = jax.nn.gelu(pre_act, approximate=True).astype(jnp.bfloat16)
        return jnp.dot(hidden, w_down, preferred_element_type=jnp.float32).astype(jnp.bfloat16)

    y_blocks = lax.map(row_block, x_blocks)
    return y_blocks.reshape(ROW_GROUPS * TOK_DEV, D)
```

```python
import jax
import jax.numpy as jnp
from jax import lax
from jax.sharding import PartitionSpec as P

ROW_AXES = ("dp", "row")
COL_AXES = ("co", "ci")
SWAP = [(0, 1), (1, 0)]


def solution(mesh):
    def over_x(a):
        return lax.ppermute(a, "co", SWAP)

    def over_y(a):
        return lax.ppermute(a, "row", SWAP)

    def over_c(a):
        return lax.ppermute(a, "ci", SWAP)

    def local_mlp(x_blk, w1, w2):
        y, x, c = lax.axis_index("row"), lax.axis_index("co"), lax.axis_index("ci")
        half = w1.shape[1] // 2
        quarter = half // 2

        x_far = over_x(x_blk)
        w1_y = [over_y(w1[:, :half]), over_y(w1[:, half:])]
        w1_x_hi = over_x(w1[:, half:])
        w1_x_lo = over_x(w1[:, :half])
        w2_far = [over_y(w2[:2048]), over_y(w2[2048:])]
        diag_lo = over_x(w1_y[0])
        diag_hi = over_y(w1_x_hi)

        def pair(a, b, first):
            return jnp.where(first == 0, jnp.concatenate([a, b], 1), jnp.concatenate([b, a], 1))

        x_near2 = over_c(x_blk)
        x_far2 = over_c(x_far)
        near = pair(x_blk, x_near2, c)
        far = pair(x_far, x_far2, c)
        same = x == y

        def hid(w_own, w_oth):
            w_near = jnp.where(same, w_own, w_oth)
            w_far = jnp.where(same, w_oth, w_own)
            p = jnp.dot(near, w_near, preferred_element_type=jnp.float32)
            p = p + jnp.dot(far, w_far, preferred_element_type=jnp.float32)
            return jax.nn.gelu(p, approximate=True).astype(jnp.bfloat16)

        def contrib(h, h2, fx, lo, n):
            w2_own_half = jnp.where(fx == y, w2, jnp.concatenate(w2_far, 0))
            wa = lax.dynamic_slice(w2_own_half, (c * 2048 + lo, 0), (n, w2.shape[1]))
            wb = lax.dynamic_slice(w2_own_half, ((1 - c) * 2048 + lo, 0), (n, w2.shape[1]))
            return (jnp.dot(h, wa, preferred_element_type=jnp.float32)
                    + jnp.dot(h2, wb, preferred_element_type=jnp.float32))

        parts = []
        for lo, own, oth, fx in (
            (0, w1[:, :half], w1_y[0], x),
            (half, w1[:, half:], w1_y[1], x),
            (0, w1_x_lo, diag_lo, 1 - x),
            (half, w1_x_hi, diag_hi, 1 - x),
        ):
            h = hid(own, oth)
            h2 = over_c(h)
            parts.append((h, h2, fx, lo, half))
        acc = None
        for p in parts:
            t = contrib(*p)
            acc = t if acc is None else acc + t
        return acc.astype(jnp.bfloat16)

    act_spec = P(ROW_AXES, COL_AXES)
    wgt_spec = P("row", COL_AXES)
    return jax.shard_map(local_mlp, mesh=mesh, in_specs=(act_spec, wgt_spec, wgt_spec), out_specs=act_spec, check_vma=False)
```

```python
import functools

import jax
import jax.numpy as jnp
from jax import lax
from jax.experimental import pallas as pl
from jax.experimental.pallas import tpu as pltpu
from jax.sharding import PartitionSpec as P

ROW_AXES = ("dp", "row")
COL_AXES = ("co", "ci")
MESH = pl.DeviceIdType.MESH
BF = jnp.bfloat16

W = 256
TT = 512

ITEMS = (
    (0, 0), (0, 1), (0, 2), (0, 3), (0, 4), (1, 4), (1, 0), (0, 5),
    (1, 5), (1, 1), (0, 6), (1, 6), (1, 2), (0, 7), (1, 7), (1, 3),
)
AHEAD = (1, 2, 3, 4, 6, 9, 12, 15)
SERVE = {
    2: ("D4", "Y4"),
    3: ("D5", "V4"),
    5: ("D0", "Y5", "B4", "A0"),
    7: ("D6", "V5"),
    8: ("D1", "Y6", "B5", "A1"),
    10: ("D7", "V6"),
    11: ("D2", "Y7", "B6", "A2"),
    13: ("D3", "V7"),
    14: ("B7", "A3"),
}


def kernel(x_in, w1, w2, y_out, ws, wy_o, wy_s, wx_o, wx_s, wd_o, wd_s, w2s, w2y_o, w2y_s,
           xs, acc, w1b, w2b, st_o, st_s, send, recv, lsem, osem):
    dp, y, x, c = (lax.axis_index(a) for a in ("dp", "row", "co", "ci"))
    tok = x_in.shape[0] // 2
    dh = w1.shape[0]
    cols = x_in.shape[1]
    sib, xn, yn = (dp, y, x, 1 - c), (dp, y, 1 - x, c), (dp, 1 - y, x, c)
    xn2 = (dp, y, 1 - x, 1 - c)

    copies = {}

    def add(name, src, dst, dev):
        i = len(copies)
        copies[name] = functools.partial(
            pltpu.make_async_remote_copy,
            src_ref=src, dst_ref=dst, send_sem=send.at[i], recv_sem=recv.at[i],
            device_id=dev, device_id_type=MESH)

    def start(*names):
        for n in names:
            copies[n]().start()

    def got(*names):
        for n in names:
            copies[n]().wait_recv()

    my_cols = pl.ds(pl.multiple_of((x * 2 + c) * cols, 128), cols)
    my_tok = pl.ds(pl.multiple_of(c * tok, TT), tok)
    sib_tok = pl.ds(pl.multiple_of((1 - c) * tok, TT), tok)
    add("Xc", x_in.at[sib_tok], xs.at[:, my_cols], sib)
    add("Xx", x_in.at[my_tok], xs.at[:, my_cols], xn)
    add("Xz", x_in.at[sib_tok], xs.at[:, my_cols], xn2)
    add("ws", w1, ws, sib)
    add("w2s", w2, w2s, sib)
    nk = w1.shape[1] // W
    for k in range(nk):
        part = w1.at[:, pl.ds(k * W, W)]
        rows = pl.ds(k * W, W)
        add(f"Y{k}", part, wy_o.at[k], yn)
        add(f"fY{k}", wy_o.at[k], wy_s.at[k], sib)
        add(f"D{k}", part, wx_o.at[k], xn)
        add(f"fD{k}", wx_o.at[k], wx_s.at[k], sib)
        add(f"V{k}", w2.at[:, rows], w2y_o.at[:, rows], yn)
        add(f"fV{k}", w2y_o.at[:, rows], w2y_s.at[:, rows], sib)
        if k < nk // 2:
            add(f"A{k}", wy_o.at[k], wd_o.at[k], xn)
            add(f"fA{k}", wd_o.at[k], wd_s.at[k], sib)
        else:
            add(f"B{k}", wx_o.at[k], wd_o.at[k], yn)
            add(f"fB{k}", wd_o.at[k], wd_s.at[k], sib)
    nt = tok // TT
    for t in range(nt):
        add(f"O{t}", st_s.at[pl.ds(t * TT, TT)], y_out.at[pl.ds(pl.multiple_of(c * tok + t * TT, TT), TT)], sib)

    def serve(name):
        got(name)
        start("f" + name)
        kind, k = name[0], int(name[1:])
        if kind == "Y" and k < nk // 2:
            start(f"A{k}")
            start(*(("D6", "D1"), ("D7", "D2"), ("D3",), ())[k])
        if kind == "D" and k >= nk // 2:
            start(f"B{k}")
            start(*(("V5", "Y6"), ("V6", "Y7"), ("V7",), ())[k - nk // 2])

    def loads(i):
        far, k = ITEMS[i]
        slot = i % 2
        part = pl.ds(k * W, W)
        if far:
            srcs = (wx_o.at[k], wd_o.at[k], wx_s.at[k], wd_s.at[k])
        else:
            srcs = (w1.at[:, part], wy_o.at[k], ws.at[:, part], wy_s.at[k])
        out = []
        for j, s in enumerate(srcs):
            rows = pl.ds(pl.multiple_of((y if j % 2 == 0 else 1 - y) * dh, 128), dh)
            lanes = pl.ds(pl.multiple_of((c if j < 2 else 1 - c) * W, 128), W)
            out.append((s, w1b.at[slot, rows, lanes], lsem.at[slot, j]))
        near, dist = ([
            (own.at[:, part], w2b.at[slot, :, :, pl.ds(0, cols)], lsem.at[slot, 4]),
            (oth.at[:, part], w2b.at[slot, :, :, pl.ds(cols, cols)], lsem.at[slot, 5]),
        ] for own, oth in ((w2, w2s), (w2y_o, w2y_s)))
        return out, near, dist

    def load(i):
        far, k = ITEMS[i]
        if far:
            got(f"fD{k}", f"fA{k}" if k < nk // 2 else f"fB{k}")
        else:
            got(f"fY{k}", f"fV{k}")
        first, near, dist = loads(i)
        for d in first:
            pltpu.make_async_copy(*d).start()
        local = (x != y) if far else (x == y)

        @pl.when(local)
        def _():
            for d in near:
                pltpu.make_async_copy(*d).start()

        @pl.when(jnp.logical_not(local))
        def _():
            for d in dist:
                pltpu.make_async_copy(*d).start()

    def loaded(i):
        first, near, _ = loads(i)
        for d in first + near:
            pltpu.make_async_copy(*d).wait()

    barrier = pltpu.get_barrier_semaphore()
    for dev in (sib, xn, xn2, yn):
        pl.semaphore_signal(barrier, inc=1, device_id=dev, device_id_type=MESH)
    pl.semaphore_wait(barrier, 4)

    start("Xx", "Y0", "Xz", "V0", "Xc", "ws", "w2s")
    own = pltpu.make_async_copy(x_in.at[my_tok], xs.at[:, my_cols], osem.at[0])
    own.start()
    start("Y1", "V1", "Y2", "V2", "Y3", "V3", "Y4", "V4", "Y5", "D4", "D5", "D0")

    @pl.loop(0, nt)
    def _(t):
        acc[pl.ds(t * TT, TT), :] = jnp.zeros((TT, acc.shape[1]), jnp.float32)

    for k in range(nk // 2):
        serve(f"Y{k}")
        serve(f"V{k}")
    own.wait()
    got("Xc", "Xx", "Xz", "ws", "w2s")

    def out_copy(t):
        rows = pl.ds(pl.multiple_of(c * tok + t * TT, TT), TT)
        return pltpu.make_async_copy(st_o.at[pl.ds(t * TT, TT)], y_out.at[rows], osem.at[1 + t])

    n_items = len(ITEMS)

    @pl.loop(0, n_items)
    def _(i):
        for n in range(n_items):
            @pl.when(i == n)
            def _():
                for name in SERVE.get(n, ()):
                    serve(name)
                if n not in AHEAD:
                    load(n)
                loaded(n)
                if n + 1 in AHEAD:
                    load(n + 1)

        slot = lax.rem(i, 2)

        @pl.loop(0, nt)
        def _(t):
            rows = pl.ds(pl.multiple_of(t * TT, TT), TT)
            p = jnp.dot(xs[rows, :], w1b[slot], preferred_element_type=jnp.float32)
            h = jax.nn.gelu(p, approximate=True).astype(BF)
            v = w2b[slot].reshape(2 * W, 2 * cols)
            acc[rows, :] += jnp.dot(h, v, preferred_element_type=jnp.float32)

    for t in range(nt):
        rows = pl.ds(t * TT, TT)
        st_s[rows, :] = acc[rows, cols:].astype(BF)
        st_o[rows, :] = acc[rows, :cols].astype(BF)
        if t:
            start(f"O{t - 1}")
            out_copy(t - 1).start()
    start(f"O{nt - 1}")
    out_copy(nt - 1).start()
    for t in range(nt):
        out_copy(t).wait()
        got(f"O{t}")
    for cp in copies.values():
        cp().wait_send()


def solution(mesh):
    def local_mlp(x_blk, w1, w2):
        rows, cols = x_blk.shape
        dh, fq = w1.shape
        tok = rows // 2
        nk = fq // W
        w2v = w2.reshape(2, fq, cols)
        land = jax.ShapeDtypeStruct((nk, dh, W), BF)
        down = jax.ShapeDtypeStruct(w2v.shape, BF)
        n_copies = 5 + 8 * nk + tok // TT
        outs = pl.pallas_call(
            kernel,
            out_shape=[jax.ShapeDtypeStruct(x_blk.shape, BF), jax.ShapeDtypeStruct(w1.shape, BF)] + [land] * 6 + [down] * 3,
            in_specs=[pl.BlockSpec(memory_space=pl.ANY)] * 3,
            out_specs=[pl.BlockSpec(memory_space=pl.ANY)] * 11,
            scratch_shapes=[
                pltpu.VMEM((tok, 4 * cols), BF),
                pltpu.VMEM((tok, 2 * cols), jnp.float32),
                pltpu.VMEM((2, 2 * dh, 2 * W), BF),
                pltpu.VMEM((2, 2, W, 2 * cols), BF),
                pltpu.VMEM((tok, cols), BF),
                pltpu.VMEM((tok, cols), BF),
                pltpu.SemaphoreType.DMA((n_copies,)),
                pltpu.SemaphoreType.DMA((n_copies,)),
                pltpu.SemaphoreType.DMA((2, 6)),
                pltpu.SemaphoreType.DMA((1 + tok // TT,)),
            ],
            compiler_params=pltpu.CompilerParams(
                collective_id=0, has_side_effects=True, vmem_limit_bytes=67_000_000),
        )(x_blk, w1, w2v)
        return outs[0]

    act_spec = P(ROW_AXES, COL_AXES)
    wgt_spec = P("row", COL_AXES)
    return jax.shard_map(local_mlp, mesh=mesh, in_specs=(act_spec, wgt_spec, wgt_spec), out_specs=act_spec, check_vma=False)
```

```python
import functools

import jax
import jax.numpy as jnp
from jax import lax
from jax.experimental import pallas as pl
from jax.experimental.pallas import tpu as pltpu
from jax.sharding import PartitionSpec as P

ROW_AXES = ("dp", "row")
COL_AXES = ("co", "ci")
MESH = pl.DeviceIdType.MESH
BF = jnp.bfloat16

W = 256
HW = W // 2
TT = 512

STEPS = (
    ("full", 0, 0), ("full", 0, 1), ("full", 0, 4), ("hid", 0, 7), ("full", 0, 5),
    ("full", 1, 4), ("full", 0, 2), ("full", 1, 5), ("full", 0, 3), ("hid", 0, 6),
    ("full", 1, 1), ("full", 1, 0), ("full", 1, 2), ("part", 1, 7), ("part", 1, 6),
    ("full", 1, 3), ("comp", 1, 0), ("comp", 1, 1), ("comp", 1, 2), ("comp", 1, 3),
)
LINK_X = (
    "Xx0", "Xz0", "Xx1", "Xz1", "Xx2", "Xz2", "Xx3", "Xz3", "A4", "D4", "D5", "A5",
    "D1", "D0", "D2", "D3", "D7", "D6", "P0", "P1", "P2", "P3",
)
LINK_Y = (
    "Y1", "Y0", "V1", "V0", "V3", "Y4", "V4", "V5", "Y7", "Y5", "Y2", "V2",
    "Y3", "Y6", "B1", "B0", "B2", "B3", "Q0", "Q1", "Q2", "Q3",
)
HOOKS = {
    0: ("Y1", "V0", "Y0", "V1", "L0",),
    1: ("L1",),
    4: ("Y4",),
    6: ("V4",),
    8: ("L2",),
    11: ("V5", "Y7",),
    12: ("L3",),
    13: ("Y5",),
    14: ("D4",),
    16: ("A4", "L4", "L5",),
    18: ("Y2",),
    20: ("V3", "D5",),
    22: ("A5",),
    23: ("V2",),
    24: ("L6", "L7",),
    27: ("D1",),
    28: ("Y3", "L8",),
    31: ("Y6",),
    32: ("D0", "L9",),
    35: ("B1", "D2",),
    36: ("L10",),
    42: ("D3", "B0",),
    43: ("L11",),
    47: ("B2", "D7", "L12",),
    51: ("L13",),
    52: ("D6", "L14",),
    53: ("B3",),
    56: ("L15",),
    59: ("Q0",),
    62: ("P0",),
    65: ("Q1",),
    66: ("P1",),
    67: ("P2",),
    68: ("Q2",),
    73: ("P3", "Q3",),
}
NT = 4
N_TILES = NT * len(STEPS)


def tile_of(b):
    return (b % 2, b // 2) if b < 2 * NT else (b // NT, b % NT)


def links_after():
    def wants(n):
        k = int(n[-1])
        return {"A": f"Y{k}", "B": f"D{k}", "P": f"Y{6 + k // 2}"}.get(n[0])

    served, at, res = set(), [0, 0], {}
    events = [None] + [n for b in sorted(HOOKS) for n in HOOKS[b] if n[0] != "L"]
    for e in events:
        served.add(e)
        new = []
        for j, link in enumerate((LINK_X, LINK_Y)):
            while at[j] < len(link) and (wants(link[at[j]]) is None or wants(link[at[j]]) in served):
                new.append(link[at[j]])
                at[j] += 1
        res[e] = tuple(new)
    assert at == [len(LINK_X), len(LINK_Y)]
    return res


NEXT = links_after()


def any_of(i, kind):
    hit = [i == n for n, s in enumerate(STEPS) if s[0] == kind]
    return functools.reduce(jnp.logical_or, hit)


def kernel(x_in, w1, w2, y_out, ws, wy_o, wy_s, wx_o, wx_s, wd_o, wd_s, w2s, w2y_o, w2y_s,
           xs, acc, w1b, w2b, p32, hn, wl, w2c, send, recv, lsem, osem, csem):
    dp, y, x, c = (lax.axis_index(a) for a in ("dp", "row", "co", "ci"))
    tok = x_in.shape[0] // 2
    dh = w1.shape[0]
    cols = x_in.shape[1]
    nk = w1.shape[1] // W
    nt = NT
    assert tok == NT * TT and nk == 8
    sib, xn, yn = (dp, y, x, 1 - c), (dp, y, 1 - x, c), (dp, 1 - y, x, c)
    xn2 = (dp, y, 1 - x, 1 - c)
    same = x == y
    v_here = jnp.where(same, 1, 0)
    v_there = 1 - v_here

    copies = {}

    def add(name, src, dst, dev):
        i = len(copies)
        copies[name] = functools.partial(
            pltpu.make_async_remote_copy,
            src_ref=src, dst_ref=dst, send_sem=send.at[i], recv_sem=recv.at[i],
            device_id=dev, device_id_type=MESH)

    def start(*names):
        for n in names:
            copies[n]().start()

    def got(*names):
        for n in names:
            copies[n]().wait_recv()

    def at(i, n, unit=128):
        return pl.ds(pl.multiple_of(i * n, unit), n)

    my_cols = at(x * 2 + c, cols)
    my_tok, sib_tok = at(c, tok), at(1 - c, tok)
    add("Xc", x_in.at[sib_tok], xs.at[:, my_cols], sib)
    for q in range(NT):
        for name, who, dev in (("Xx", c, xn), ("Xz", 1 - c, xn2)):
            src = x_in.at[pl.ds(pl.multiple_of(who * tok + q * TT, TT), TT)]
            add(f"{name}{q}", src, xs.at[pl.ds(q * TT, TT), my_cols], dev)
    add("ws", w1, ws, sib)
    add("w2s", w2, w2s, sib)
    for k in range(nk):
        part = pl.ds(k * W, W)
        add(f"Y{k}", w1.at[:, part], wy_o.at[k], yn)
        add(f"fY{k}", wy_o.at[k], wy_s.at[k], sib)
        add(f"D{k}", w1.at[:, part], wx_o.at[k], xn)
        add(f"fD{k}", wx_o.at[k], wx_s.at[k], sib)
        if k < 6:
            add(f"V{k}", w2.at[:, part], w2y_o.at[:, part], yn)
            add(f"fV{k}", w2y_o.at[:, part], w2y_s.at[:, part], sib)
            way = ("B", wx_o, yn) if k < 4 else ("A", wy_o, xn)
            add(f"{way[0]}{k}", way[1].at[k], wd_o.at[k], way[2])
            add(f"f{way[0]}{k}", wd_o.at[k], wd_s.at[k], sib)
    for h in range(4):
        k, half = 6 + h // 2, pl.ds((h % 2) * HW, HW)
        rows = pl.ds(k * W + (h % 2) * HW, HW)
        mine = wl.at[h, :, at(c, HW)]
        add(f"P{h}", wy_o.at[k, :, half], mine, xn)
        add(f"fP{h}", mine, mine, sib)
        left, right = pl.ds(0, cols), pl.ds(cols, cols)
        add(f"Q{h}", w2.at[:, rows], w2c.at[h, v_there, :, :, left], yn)
        add(f"fQ{h}", w2c.at[h, v_here, :, :, left], w2c.at[h, v_here, :, :, right], sib)
    o_base = len(copies)

    def out_copies(t):
        rows = pl.ds(pl.multiple_of(t * TT, TT), TT)
        there = pl.ds(pl.multiple_of(c * tok + t * TT, TT), TT)
        return [pltpu.make_async_remote_copy(
            src_ref=hn.at[j, rows], dst_ref=y_out.at[there, pl.ds(j * W, W)],
            send_sem=send.at[o_base + 3 * t + j], recv_sem=recv.at[o_base + 3 * t + j],
            device_id=sib, device_id_type=MESH) for j in range(3)]

    def serve(name):
        got(name)
        start("f" + name)
        start(*NEXT.get(name, ()))

    def w1_loads(i):
        kind, far, k = STEPS[i]
        slot = i % 2
        part = pl.ds(k * W, W)
        if far:
            srcs = (wx_o.at[k], wd_o.at[k], wx_s.at[k], wd_s.at[k])
        else:
            srcs = (w1.at[:, part], wy_o.at[k], ws.at[:, part], wy_s.at[k])
        out = []
        for j, s in enumerate(srcs):
            rows = at(y if j % 2 == 0 else 1 - y, dh)
            who = c if j < 2 else 1 - c
            if kind == "full":
                out.append((s, w1b.at[slot, rows, at(who, W)], lsem.at[slot, j]))
            elif kind == "hid" or j % 2 == 0:
                for b in range(2):
                    lanes = pl.ds(pl.multiple_of(b * W + who * HW, 128), HW)
                    out.append((s.at[:, pl.ds(b * HW, HW)], w1b.at[slot, rows, lanes], lsem.at[slot, 2 * j + b]))
        return out

    def w2_loads(i, own, oth):
        _, far, k = STEPS[i]
        slot, part = i % 2, pl.ds(k * W, W)
        return [(own.at[:, part], w2b.at[slot, :, :, pl.ds(0, cols)], lsem.at[slot, 8]),
                (oth.at[:, part], w2b.at[slot, :, :, pl.ds(cols, cols)], lsem.at[slot, 9])]

    have_v = set()

    def begin(many):
        for d in many:
            pltpu.make_async_copy(*d).start()

    def load(i):
        kind, far, k = STEPS[i]
        if kind == "comp":
            return
        if far:
            got(f"fD{k}")
            if kind == "full":
                got(f"fB{k}" if k < 4 else f"fA{k}")
        else:
            got(f"fY{k}")
        if kind == "full" and k not in have_v:
            have_v.add(k)
            got(f"fV{k}")
        begin(w1_loads(i))
        if kind == "full":
            local = jnp.logical_not(same) if far else same

            @pl.when(local)
            def _():
                begin(w2_loads(i, w2, w2s))

            @pl.when(jnp.logical_not(local))
            def _():
                begin(w2_loads(i, w2y_o, w2y_s))

    def loaded(i):
        kind, _, k = STEPS[i]
        if kind == "comp":
            got(f"fP{k}", f"fQ{k}")
            return
        for d in w1_loads(i) + (w2_loads(i, w2, w2s) if kind == "full" else []):
            pltpu.make_async_copy(*d).wait()

    barrier = pltpu.get_barrier_semaphore()
    for dev in (sib, xn, xn2, yn):
        pl.semaphore_signal(barrier, inc=1, device_id=dev, device_id_type=MESH)
    pl.semaphore_wait(barrier, 4)

    first = NEXT[None]
    start(*first[:1], "Xc", "ws", "w2s", *first[1:])
    own = pltpu.make_async_copy(x_in.at[my_tok], xs.at[:, my_cols], osem)
    own.start()

    keep = []
    for h in range(4):
        rows = pl.ds((6 + h // 2) * W + (h % 2) * HW, HW)
        for j, src in enumerate((w2, w2s)):
            keep.append((src.at[:, rows], w2c.at[h, v_there, :, :, pl.ds(j * cols, cols)], csem.at[h, j]))
    begin(keep[::2])

    @pl.loop(0, nt)
    def _(t):
        acc[pl.ds(t * TT, TT), :] = jnp.zeros((TT, acc.shape[1]), jnp.float32)

    got("ws", "w2s")
    begin(keep[1::2])
    for d in keep:
        pltpu.make_async_copy(*d).wait()
    own.wait()
    got("Xc")

    n_steps = len(STEPS)
    f32 = jnp.float32

    def before(b):
        i, t = tile_of(b)
        for name in HOOKS.get(b, ()):
            if name[0] == "L":
                load(int(name[1:]))
            else:
                serve(name)
        if t == 0:
            loaded(i)
        if i == 0:
            got(f"Xx{t}", f"Xz{t}")

    @pl.loop(0, N_TILES)
    def _(b):
        for g in range(0, N_TILES, 8):
            @pl.when(jnp.logical_and(b >= g, b < g + 8))
            def _():
                for n in range(g, g + 8):
                    if n in HOOKS or tile_of(n)[0] == 0 or tile_of(n)[1] == 0:
                        pl.when(b == n)(functools.partial(before, n))

        early = b < 2 * NT
        i = jnp.where(early, lax.rem(b, 2), b // NT)
        t = jnp.where(early, b // 2, lax.rem(b, NT))
        slot = lax.rem(i, 2)
        rows = at(t, TT, TT)

        @pl.when(any_of(i, "full"))
        def _():
            p = jnp.dot(xs[rows, :], w1b[slot], preferred_element_type=f32)
            h = jax.nn.gelu(p, approximate=True).astype(BF)
            v = w2b[slot].reshape(2 * W, 2 * cols)
            acc[rows, :] += jnp.dot(h, v, preferred_element_type=f32)

        @pl.when(any_of(i, "hid"))
        def _():
            k2 = 2 * (i == STEPS.index(("hid", 0, 7))).astype(jnp.int32)

            p = jnp.dot(xs[rows, :], w1b[slot], preferred_element_type=f32)
            h = jax.nn.gelu(p, approximate=True).astype(BF)
            hn[k2, rows, :] = h[:, :W]
            hn[k2 + 1, rows, :] = h[:, W:]

        @pl.when(any_of(i, "part"))
        def _():
            k2 = 2 * (i == STEPS.index(("part", 1, 7))).astype(jnp.int32)

            p = jnp.dot(xs[rows, at(y, dh)], w1b[slot, at(y, dh), :], preferred_element_type=f32)
            p32[k2, rows, :] = p[:, :W]
            p32[k2 + 1, rows, :] = p[:, W:]

        @pl.when(any_of(i, "comp"))
        def _():
            j = i - (n_steps - 4)

            p = p32[j, rows, :] + jnp.dot(xs[rows, at(1 - y, dh)], wl[j], preferred_element_type=f32)
            h = jax.nn.gelu(p, approximate=True).astype(BF)
            h = jnp.concatenate([hn[j, rows, :], h], axis=1)
            total = acc[rows, :] + jnp.dot(h, w2c[j].reshape(4 * HW, 2 * cols), preferred_element_type=f32)
            acc[rows, :] = total

            @pl.when(j == 3)
            def _():
                y_out[pl.ds(pl.multiple_of(c * tok + t * TT, TT), TT), :] = acc[rows, :cols].astype(BF)
                for q in range(3):
                    hn[q, rows, :] = acc[rows, cols + q * W:cols + (q + 1) * W].astype(BF)

                @pl.when(t > 0)
                def _():
                    for d in out_copies(t - 1):
                        d.start()

    for d in out_copies(nt - 1):
        d.start()
    for cp in copies.values():
        cp().wait_send()
    for t in range(nt):
        for d in out_copies(t):
            d.wait()


def solution(mesh):
    def local_mlp(x_blk, w1, w2):
        rows, cols = x_blk.shape
        dh, fq = w1.shape
        tok = rows // 2
        nk = fq // W
        w2v = w2.reshape(2, fq, cols)
        land = jax.ShapeDtypeStruct((nk, dh, W), BF)
        down = jax.ShapeDtypeStruct(w2v.shape, BF)
        n_copies = 3 + 2 * NT + 4 * nk + 4 * 6 + 16 + 3 * NT
        dma = pltpu.SemaphoreType.DMA
        outs = pl.pallas_call(
            kernel,
            out_shape=[pltpu.VMEM(x_blk.shape, BF), jax.ShapeDtypeStruct(w1.shape, BF)] + [land] * 6 + [down] * 3,
            in_specs=[pl.BlockSpec(memory_space=pl.ANY)] * 3,
            out_specs=[pl.BlockSpec(memory_space=pltpu.VMEM)] + [pl.BlockSpec(memory_space=pl.ANY)] * 10,
            scratch_shapes=[
                pltpu.VMEM((tok, 4 * cols), BF),
                pltpu.VMEM((tok, 2 * cols), jnp.float32),
                pltpu.VMEM((2, 2 * dh, 2 * W), BF),
                pltpu.VMEM((2, 2, W, 2 * cols), BF),
                pltpu.VMEM((4, tok, W), jnp.float32),
                pltpu.VMEM((4, tok, W), BF),
                pltpu.VMEM((4, dh, W), BF),
                pltpu.VMEM((4, 2, 2, HW, 2 * cols), BF),
                dma((n_copies,)), dma((n_copies,)), dma((2, 10)), dma, dma((4, 2)),
            ],
            compiler_params=pltpu.CompilerParams(
                collective_id=0, has_side_effects=True, vmem_limit_bytes=60_700_000),
        )(x_blk, w1, w2v)
        return outs[0]

    act_spec = P(ROW_AXES, COL_AXES)
    wgt_spec = P("row", COL_AXES)
    return jax.shard_map(local_mlp, mesh=mesh, in_specs=(act_spec, wgt_spec, wgt_spec), out_specs=act_spec, check_vma=False)
```

```python
import functools

import jax
import jax.numpy as jnp
from jax import lax
from jax.experimental import pallas as pl
from jax.experimental.pallas import tpu as pltpu
from jax.sharding import PartitionSpec as P

ROW_AXES = ("dp", "row")
COL_AXES = ("co", "ci")
MESH = pl.DeviceIdType.MESH
BF = jnp.bfloat16
GELU_A = 0.7978845608028654

W = 256
HW = W // 2
TT = 512
ST = TT // 2

STEPS = (
    ("full", 0, 0), ("full", 0, 1), ("full", 0, 4), ("hid", 0, 7), ("full", 0, 5),
    ("full", 1, 4), ("full", 0, 2), ("full", 1, 5), ("full", 0, 3), ("hid", 0, 6),
    ("full", 1, 1), ("full", 1, 0), ("full", 1, 2), ("part", 1, 7), ("part", 1, 6),
    ("full", 1, 3), ("comp", 1, 0), ("comp", 1, 1), ("comp", 1, 2), ("comp", 1, 3),
)
LINK_X = (
    "Xx0", "Xz0", "Xx1", "Xz1", "Xx2", "Xz2", "Xx3", "Xz3", "A4", "D4", "D5", "A5",
    "D1", "D0", "D2", "D3", "D7", "D6", "P0", "P1", "P2", "P3",
)
LINK_Y = (
    "Y1", "Y0", "V1", "V0", "V3", "Y4", "V4", "V5", "Y7", "Y5", "Y2", "V2",
    "Y3", "Y6", "B1", "B0", "B2", "B3", "Q0", "Q1", "Q2", "Q3",
)
HOOKS = {
    0: ("Y1", "V0", "Y0", "V1", "L0",),
    1: ("L1",),
    4: ("Y4",),
    6: ("V4",),
    8: ("L2",),
    11: ("V5", "Y7",),
    12: ("L3",),
    13: ("Y5",),
    14: ("D4",),
    16: ("A4", "L4", "L5",),
    18: ("Y2",),
    20: ("V3", "D5",),
    22: ("A5",),
    23: ("V2",),
    24: ("L6", "L7",),
    27: ("D1",),
    28: ("Y3", "L8",),
    31: ("Y6",),
    32: ("D0", "L9",),
    35: ("B1", "D2",),
    36: ("L10",),
    42: ("D3", "B0",),
    43: ("L11",),
    47: ("B2", "D7", "L12",),
    51: ("L13",),
    52: ("D6", "L14",),
    53: ("B3",),
    56: ("L15",),
    59: ("Q0",),
    62: ("P0",),
    65: ("Q1",),
    66: ("P1",),
    67: ("P2",),
    68: ("Q2",),
    73: ("P3", "Q3",),
}
NT = 4
N_TILES = NT * len(STEPS)


def tile_of(b):
    return (b % 2, b // 2) if b < 2 * NT else (b // NT, b % NT)


def links_after():
    def wants(n):
        k = int(n[-1])
        return {"A": f"Y{k}", "B": f"D{k}", "P": f"Y{6 + k // 2}"}.get(n[0])

    served, at, res = set(), [0, 0], {}
    events = [None] + [n for b in sorted(HOOKS) for n in HOOKS[b] if n[0] != "L"]
    for e in events:
        served.add(e)
        new = []
        for j, link in enumerate((LINK_X, LINK_Y)):
            while at[j] < len(link) and (wants(link[at[j]]) is None or wants(link[at[j]]) in served):
                new.append(link[at[j]])
                at[j] += 1
        res[e] = tuple(new)
    assert at == [len(LINK_X), len(LINK_Y)]
    return res


NEXT = links_after()


def is_kind(i, kind):
    mask = sum(1 << n for n, s in enumerate(STEPS) if s[0] == kind)
    return lax.rem(lax.shift_right_logical(jnp.int32(mask), i), 2) == 1


def gelu(p):
    u = p * (GELU_A + (GELU_A * 0.044715) * (p * p))
    return (0.5 * p) * (1.0 + jnp.tanh(u))


def kernel(x_in, w1, w2, y_out, ws, wy_o, wy_s, wx_o, wx_s, wd_o, wd_s, w2s, w2y_o, w2y_s,
           xs, acc, w1b, w2b, p32, hn, wl, w2c, send, recv, lsem, osem, csem):
    dp, y, x, c = (lax.axis_index(a) for a in ("dp", "row", "co", "ci"))
    tok = x_in.shape[0] // 2
    dh = w1.shape[0]
    cols = x_in.shape[1]
    nk = w1.shape[1] // W
    nt = NT
    assert tok == NT * TT and nk == 8
    sib, xn, yn = (dp, y, x, 1 - c), (dp, y, 1 - x, c), (dp, 1 - y, x, c)
    xn2 = (dp, y, 1 - x, 1 - c)
    same = x == y
    v_here = jnp.where(same, 1, 0)
    v_there = 1 - v_here

    copies = {}

    def add(name, src, dst, dev):
        i = len(copies)
        copies[name] = functools.partial(
            pltpu.make_async_remote_copy,
            src_ref=src, dst_ref=dst, send_sem=send.at[i], recv_sem=recv.at[i],
            device_id=dev, device_id_type=MESH)

    def start(*names):
        for n in names:
            copies[n]().start()

    def got(*names):
        for n in names:
            copies[n]().wait_recv()

    def at(i, n, unit=128):
        return pl.ds(pl.multiple_of(i * n, unit), n)

    my_cols = at(x * 2 + c, cols)
    my_tok, sib_tok = at(c, tok), at(1 - c, tok)
    add("Xc", x_in.at[sib_tok], xs.at[:, my_cols], sib)
    for q in range(NT):
        for name, who, dev in (("Xx", c, xn), ("Xz", 1 - c, xn2)):
            src = x_in.at[pl.ds(pl.multiple_of(who * tok + q * TT, TT), TT)]
            add(f"{name}{q}", src, xs.at[pl.ds(q * TT, TT), my_cols], dev)
    add("ws", w1, ws, sib)
    add("w2s", w2, w2s, sib)
    for k in range(nk):
        part = pl.ds(k * W, W)
        add(f"Y{k}", w1.at[:, part], wy_o.at[k], yn)
        add(f"fY{k}", wy_o.at[k], wy_s.at[k], sib)
        add(f"D{k}", w1.at[:, part], wx_o.at[k], xn)
        add(f"fD{k}", wx_o.at[k], wx_s.at[k], sib)
        if k < 6:
            add(f"V{k}", w2.at[:, part], w2y_o.at[:, part], yn)
            add(f"fV{k}", w2y_o.at[:, part], w2y_s.at[:, part], sib)
            way = ("B", wx_o, yn) if k < 4 else ("A", wy_o, xn)
            add(f"{way[0]}{k}", way[1].at[k], wd_o.at[k], way[2])
            add(f"f{way[0]}{k}", wd_o.at[k], wd_s.at[k], sib)
    for h in range(4):
        k, half = 6 + h // 2, pl.ds((h % 2) * HW, HW)
        rows = pl.ds(k * W + (h % 2) * HW, HW)
        mine = wl.at[h, :, at(c, HW)]
        add(f"P{h}", wy_o.at[k, :, half], mine, xn)
        add(f"fP{h}", mine, mine, sib)
        left, right = pl.ds(0, cols), pl.ds(cols, cols)
        add(f"Q{h}", w2.at[:, rows], w2c.at[h, v_there, :, :, left], yn)
        add(f"fQ{h}", w2c.at[h, v_here, :, :, left], w2c.at[h, v_here, :, :, right], sib)
    o_base = len(copies)

    def out_copies(t):
        rows = pl.ds(pl.multiple_of(t * TT, TT), TT)
        there = pl.ds(pl.multiple_of(c * tok + t * TT, TT), TT)
        return [pltpu.make_async_remote_copy(
            src_ref=hn.at[j, rows], dst_ref=y_out.at[there, pl.ds(j * W, W)],
            send_sem=send.at[o_base + 3 * t + j], recv_sem=recv.at[o_base + 3 * t + j],
            device_id=sib, device_id_type=MESH) for j in range(3)]

    def serve(name):
        got(name)
        start("f" + name)
        start(*NEXT.get(name, ()))

    def w1_loads(i):
        kind, far, k = STEPS[i]
        slot = i % 2
        part = pl.ds(k * W, W)
        if far:
            srcs = (wx_o.at[k], wd_o.at[k], wx_s.at[k], wd_s.at[k])
        else:
            srcs = (w1.at[:, part], wy_o.at[k], ws.at[:, part], wy_s.at[k])
        out = []
        for j, s in enumerate(srcs):
            rows = at(y if j % 2 == 0 else 1 - y, dh)
            who = c if j < 2 else 1 - c
            if kind == "full":
                out.append((s, w1b.at[slot, rows, at(who, W)], lsem.at[slot, j]))
            elif kind == "hid" or j % 2 == 0:
                for b in range(2):
                    lanes = pl.ds(pl.multiple_of(b * W + who * HW, 128), HW)
                    out.append((s.at[:, pl.ds(b * HW, HW)], w1b.at[slot, rows, lanes], lsem.at[slot, 2 * j + b]))
        return out

    def w2_loads(i, own, oth):
        _, far, k = STEPS[i]
        slot, part = i % 2, pl.ds(k * W, W)
        return [(own.at[:, part], w2b.at[slot, :, :, pl.ds(0, cols)], lsem.at[slot, 8]),
                (oth.at[:, part], w2b.at[slot, :, :, pl.ds(cols, cols)], lsem.at[slot, 9])]

    have_v = set()

    def begin(many):
        for d in many:
            pltpu.make_async_copy(*d).start()

    def load(i):
        kind, far, k = STEPS[i]
        if kind == "comp":
            return
        if far:
            got(f"fD{k}")
            if kind == "full":
                got(f"fB{k}" if k < 4 else f"fA{k}")
        else:
            got(f"fY{k}")
        if kind == "full" and k not in have_v:
            have_v.add(k)
            got(f"fV{k}")
        begin(w1_loads(i))
        if kind == "full":
            local = jnp.logical_not(same) if far else same

            @pl.when(local)
            def _():
                begin(w2_loads(i, w2, w2s))

            @pl.when(jnp.logical_not(local))
            def _():
                begin(w2_loads(i, w2y_o, w2y_s))

    def loaded(i):
        kind, _, k = STEPS[i]
        if kind == "comp":
            got(f"fP{k}", f"fQ{k}")
            return
        for d in w1_loads(i) + (w2_loads(i, w2, w2s) if kind == "full" else []):
            pltpu.make_async_copy(*d).wait()

    barrier = pltpu.get_barrier_semaphore()
    for dev in (sib, xn, xn2, yn):
        pl.semaphore_signal(barrier, inc=1, device_id=dev, device_id_type=MESH)
    pl.semaphore_wait(barrier, 4)

    first = NEXT[None]
    start(*first[:1], "Xc", "ws", "w2s", *first[1:])
    own = pltpu.make_async_copy(x_in.at[my_tok], xs.at[:, my_cols], osem)
    own.start()

    keep = []
    for h in range(4):
        rows = pl.ds((6 + h // 2) * W + (h % 2) * HW, HW)
        for j, src in enumerate((w2, w2s)):
            keep.append((src.at[:, rows], w2c.at[h, v_there, :, :, pl.ds(j * cols, cols)], csem.at[h, j]))
    begin(keep[::2])

    @pl.loop(0, nt)
    def _(t):
        acc[pl.ds(t * TT, TT), :] = jnp.zeros((TT, acc.shape[1]), jnp.float32)

    got("ws", "w2s")
    begin(keep[1::2])
    for d in keep:
        pltpu.make_async_copy(*d).wait()
    own.wait()
    got("Xc")

    n_steps = len(STEPS)
    f32 = jnp.float32

    def before(b):
        i, t = tile_of(b)
        for name in HOOKS.get(b, ()):
            if name[0] == "L":
                load(int(name[1:]))
            else:
                serve(name)
        if t == 0:
            loaded(i)
        if i == 0:
            got(f"Xx{t}", f"Xz{t}")

    @pl.loop(0, N_TILES)
    def _(b):
        def pick(lo, hi):
            if not any(n in busy for n in range(lo, hi)):
                return lambda: None
            if hi - lo == 1:
                return functools.partial(before, lo)
            mid = (lo + hi) // 2
            low, high = pick(lo, mid), pick(mid, hi)
            return lambda: lax.cond(b < mid, low, high)

        busy = [n for n in range(N_TILES) if n in HOOKS or tile_of(n)[0] == 0 or tile_of(n)[1] == 0]
        pick(0, N_TILES)()

        early = b < 2 * NT
        i = jnp.where(early, lax.rem(b, 2), b // NT)
        t = jnp.where(early, b // 2, lax.rem(b, NT))
        slot = lax.rem(i, 2)
        rows = at(t, TT, TT)

        subs = [pl.ds(pl.multiple_of(t * TT + q * ST, ST), ST) for q in range(TT // ST)]

        @pl.when(is_kind(i, "full"))
        def _():
            ps = [jnp.dot(xs[r, :], w1b[slot], preferred_element_type=f32) for r in subs]
            for r, p in zip(subs, ps):
                h = gelu(p).astype(BF)
                v = w2b[slot].reshape(2 * W, 2 * cols)
                acc[r, :] += jnp.dot(h, v, preferred_element_type=f32)

        @pl.when(is_kind(i, "hid"))
        def _():
            k2 = 2 * (i == STEPS.index(("hid", 0, 7))).astype(jnp.int32)
            ps = [jnp.dot(xs[r, :], w1b[slot], preferred_element_type=f32) for r in subs]
            for r, p in zip(subs, ps):
                h = gelu(p).astype(BF)
                hn[k2, r, :] = h[:, :W]
                hn[k2 + 1, r, :] = h[:, W:]

        @pl.when(is_kind(i, "part"))
        def _():
            k2 = 2 * (i == STEPS.index(("part", 1, 7))).astype(jnp.int32)
            p = jnp.dot(xs[rows, at(y, dh)], w1b[slot, at(y, dh), :], preferred_element_type=f32)
            p32[k2, rows, :] = p[:, :W]
            p32[k2 + 1, rows, :] = p[:, W:]

        def comp(j):
            ps = [p32[j, r, :] + jnp.dot(xs[r, at(1 - y, dh)], wl[j], preferred_element_type=f32) for r in subs]
            for r, p in zip(subs, ps):
                h = jnp.concatenate([hn[j, r, :], gelu(p).astype(BF)], axis=1)
                v = w2c[j].reshape(4 * HW, 2 * cols)
                yield r, acc[r, :] + jnp.dot(h, v, preferred_element_type=f32)

        last = i == n_steps - 1

        @pl.when(jnp.logical_and(is_kind(i, "comp"), jnp.logical_not(last)))
        def _():
            for r, total in comp(i - (n_steps - 4)):
                acc[r, :] = total

        @pl.when(last)
        def _():
            for q, (r, total) in enumerate(comp(3)):
                y_out[pl.ds(pl.multiple_of(c * tok + t * TT + q * ST, ST), ST), :] = total[:, :cols].astype(BF)
                for m in range(3):
                    hn[m, r, :] = total[:, cols + m * W:cols + (m + 1) * W].astype(BF)

            @pl.when(t > 0)
            def _():
                for d in out_copies(t - 1):
                    d.start()

    for d in out_copies(nt - 1):
        d.start()
    for cp in copies.values():
        cp().wait_send()
    for t in range(nt):
        for d in out_copies(t):
            d.wait()


def solution(mesh):
    def local_mlp(x_blk, w1, w2):
        rows, cols = x_blk.shape
        dh, fq = w1.shape
        tok = rows // 2
        nk = fq // W
        w2v = w2.reshape(2, fq, cols)
        land = jax.ShapeDtypeStruct((nk, dh, W), BF)
        down = jax.ShapeDtypeStruct(w2v.shape, BF)
        n_copies = 3 + 2 * NT + 4 * nk + 4 * 6 + 16 + 3 * NT
        dma = pltpu.SemaphoreType.DMA
        outs = pl.pallas_call(
            kernel,
            out_shape=[pltpu.VMEM(x_blk.shape, BF), jax.ShapeDtypeStruct(w1.shape, BF)] + [land] * 6 + [down] * 3,
            in_specs=[pl.BlockSpec(memory_space=pl.ANY)] * 3,
            out_specs=[pl.BlockSpec(memory_space=pltpu.VMEM)] + [pl.BlockSpec(memory_space=pl.ANY)] * 10,
            scratch_shapes=[
                pltpu.VMEM((tok, 4 * cols), BF),
                pltpu.VMEM((tok, 2 * cols), jnp.float32),
                pltpu.VMEM((2, 2 * dh, 2 * W), BF),
                pltpu.VMEM((2, 2, W, 2 * cols), BF),
                pltpu.VMEM((4, tok, W), jnp.float32),
                pltpu.VMEM((4, tok, W), BF),
                pltpu.VMEM((4, dh, W), BF),
                pltpu.VMEM((4, 2, 2, HW, 2 * cols), BF),
                dma((n_copies,)), dma((n_copies,)), dma((2, 10)), dma, dma((4, 2)),
            ],
            compiler_params=pltpu.CompilerParams(
                collective_id=0, has_side_effects=True, vmem_limit_bytes=60_700_000),
        )(x_blk, w1, w2v)
        return outs[0]

    act_spec = P(ROW_AXES, COL_AXES)
    wgt_spec = P("row", COL_AXES)
    return jax.shard_map(local_mlp, mesh=mesh, in_specs=(act_spec, wgt_spec, wgt_spec), out_specs=act_spec, check_vma=False)
```

```python
import functools

import jax
import jax.numpy as jnp
from jax import lax
from jax.experimental import pallas as pl
from jax.experimental.pallas import tpu as pltpu
from jax.sharding import PartitionSpec as P

ROW_AXES = ("dp", "row")
COL_AXES = ("co", "ci")
MESH = pl.DeviceIdType.MESH
BF = jnp.bfloat16
GELU_A = 0.7978845608028654

W = 256
HW = W // 2
TT = 512
ST = TT // 2

STEPS = (
    ("hid", 0, 6, 0, 3), ("hid", 0, 7, 0, 3), ("full", 0, 1, 0, 4), ("full", 0, 5, 0, 3),
    ("hid", 0, 7, 3, 4), ("full", 0, 3, 0, 4), ("full", 0, 5, 3, 4), ("full", 0, 4, 1, 4),
    ("hid", 0, 6, 3, 4), ("full", 0, 4, 0, 1), ("full", 1, 5, 0, 4), ("full", 0, 0, 0, 4),
    ("full", 1, 4, 2, 4), ("full", 1, 4, 0, 1), ("full", 0, 2, 0, 4), ("full", 1, 3, 0, 4),
    ("full", 1, 4, 1, 2), ("full", 1, 2, 0, 4), ("full", 1, 0, 0, 4), ("part", 1, 6, 0, 4),
    ("full", 1, 1, 0, 4), ("part", 1, 7, 0, 4), ("comp", 1, 0, 0, 4), ("comp", 1, 1, 0, 4),
    ("comp", 1, 2, 0, 4), ("last", 1, 3, 0, 4), ("own", 1, 3, 0, 4),
)
LINK_X = (
    "Xx1", "Xx2", "Xz0", "Xz2", "Xz1", "Xx0", "Xz3", "D5", "Xx3", "A5", "D4", "D3",
    "A4", "D2", "D0", "D1", "D6", "P0", "D7", "P1", "P2", "P3",
)
LINK_Y = (
    "Y6", "V3", "V1", "Y1", "Y5", "Y7", "V5", "Y3", "Y4", "V4", "V0", "Y0",
    "V2", "Y2", "B3", "B2", "B0", "B1", "Q0", "Q1", "Q2", "Q3",
)
HOOKS = {
    0: ("Y7", "Y6", "V1", "Y1", "L0",),
    1: ("Y5",),
    2: ("L1",),
    3: ("L2",),
    6: ("V5",),
    7: ("L3",),
    8: ("Y3",),
    10: ("Y4",),
    12: ("V3", "L4",),
    13: ("L5",),
    14: ("D5",),
    15: ("L6",),
    16: ("V4",),
    18: ("L7",),
    19: ("A5",),
    21: ("V0", "L8",),
    22: ("Y0", "D4", "L9",),
    23: ("L10",),
    27: ("D3", "L11",),
    28: ("V2", "A4",),
    30: ("L12",),
    32: ("L13",),
    33: ("D2",),
    34: ("Y2", "L14",),
    38: ("B3", "L15",),
    40: ("L16",),
    41: ("D0",),
    42: ("B2",),
    43: ("L17",),
    44: ("D1",),
    47: ("B0", "D6", "L18",),
    51: ("L19",),
    52: ("B1",),
    53: ("P0",),
    54: ("L20",),
    58: ("D7",),
    59: ("L21",),
    60: ("Q0",),
    62: ("Q1",),
    64: ("P1",),
    68: ("Q2",),
    69: ("P2",),
    74: ("P3", "Q3",),
}
NT = 4
TILES = [(i, t) for i, s in enumerate(STEPS) for t in range(s[3], s[4])]
N_TILES = len(TILES)
FIRST = [TILES.index((i, s[3])) for i, s in enumerate(STEPS)]
NEW_X = [min(b for b in range(N_TILES) if TILES[b][1] == t) for t in range(NT)]


def step_and_tile(b):
    i = off = jnp.int32(0)
    for n in range(1, len(STEPS)):
        begun = (b >= FIRST[n]).astype(jnp.int32)
        i += begun
        off += begun * ((FIRST[n] - STEPS[n][3]) - (FIRST[n - 1] - STEPS[n - 1][3]))
    return i, b + STEPS[0][3] - off


def links_after():
    def wants(n):
        k = int(n[-1])
        return {"A": f"Y{k}", "B": f"D{k}", "P": f"Y{6 + k // 2}"}.get(n[0])

    served, at, res = set(), [0, 0], {}
    events = [None] + [n for b in sorted(HOOKS) for n in HOOKS[b] if n[0] != "L"]
    for e in events:
        served.add(e)
        new = []
        for j, link in enumerate((LINK_X, LINK_Y)):
            while at[j] < len(link) and (wants(link[at[j]]) is None or wants(link[at[j]]) in served):
                new.append(link[at[j]])
                at[j] += 1
        res[e] = tuple(new)
    assert at == [len(LINK_X), len(LINK_Y)]
    return res


NEXT = links_after()


def is_kind(i, kind):
    mask = sum(1 << n for n, s in enumerate(STEPS) if s[:len(kind)] == kind)
    return lax.rem(lax.shift_right_logical(jnp.int32(mask), i), 2) == 1


def gelu(p):
    u = p * (GELU_A + (GELU_A * 0.044715) * (p * p))
    return (0.5 * p) * (1.0 + jnp.tanh(u))


def kernel(x_in, w1, w2, y_out, ws, wy_o, wy_s, wx_o, wx_s, wd_o, wd_s, w2s, w2y_o, w2y_s,
           xs, acc, w1b, w2b, p32, hn, wl, w2c, send, recv, lsem, osem, csem):
    dp, y, x, c = (lax.axis_index(a) for a in ("dp", "row", "co", "ci"))
    tok = x_in.shape[0] // 2
    dh = w1.shape[0]
    cols = x_in.shape[1]
    nk = w1.shape[1] // W
    nt = NT
    assert tok == NT * TT and nk == 8
    sib, xn, yn = (dp, y, x, 1 - c), (dp, y, 1 - x, c), (dp, 1 - y, x, c)
    xn2 = (dp, y, 1 - x, 1 - c)
    same = x == y
    v_here = jnp.where(same, 1, 0)
    v_there = 1 - v_here

    copies = {}

    def add(name, src, dst, dev):
        i = len(copies)
        copies[name] = functools.partial(
            pltpu.make_async_remote_copy,
            src_ref=src, dst_ref=dst, send_sem=send.at[i], recv_sem=recv.at[i],
            device_id=dev, device_id_type=MESH)

    def start(*names):
        for n in names:
            copies[n]().start()

    def got(*names):
        for n in names:
            copies[n]().wait_recv()

    def at(i, n, unit=128):
        return pl.ds(pl.multiple_of(i * n, unit), n)

    my_cols = at(x * 2 + c, cols)
    my_tok, sib_tok = at(c, tok), at(1 - c, tok)
    add("Xc", x_in.at[sib_tok], xs.at[:, my_cols], sib)
    for q in range(NT):
        for name, who, dev in (("Xx", c, xn), ("Xz", 1 - c, xn2)):
            src = x_in.at[pl.ds(pl.multiple_of(who * tok + q * TT, TT), TT)]
            add(f"{name}{q}", src, xs.at[pl.ds(q * TT, TT), my_cols], dev)
    add("ws", w1, ws, sib)
    add("w2s", w2, w2s, sib)
    for k in range(nk):
        part = pl.ds(k * W, W)
        add(f"Y{k}", w1.at[:, part], wy_o.at[k], yn)
        add(f"fY{k}", wy_o.at[k], wy_s.at[k], sib)
        add(f"D{k}", w1.at[:, part], wx_o.at[k], xn)
        add(f"fD{k}", wx_o.at[k], wx_s.at[k], sib)
        if k < 6:
            add(f"V{k}", w2.at[:, part], w2y_o.at[:, part], yn)
            add(f"fV{k}", w2y_o.at[:, part], w2y_s.at[:, part], sib)
            way = ("B", wx_o, yn) if k < 4 else ("A", wy_o, xn)
            add(f"{way[0]}{k}", way[1].at[k], wd_o.at[k], way[2])
            add(f"f{way[0]}{k}", wd_o.at[k], wd_s.at[k], sib)
    for h in range(4):
        k, half = 6 + h // 2, pl.ds((h % 2) * HW, HW)
        rows = pl.ds(k * W + (h % 2) * HW, HW)
        mine = wl.at[h, :, at(c, HW)]
        add(f"P{h}", wy_o.at[k, :, half], mine, xn)
        add(f"fP{h}", mine, mine, sib)
        left, right = pl.ds(0, cols), pl.ds(cols, cols)
        add(f"Q{h}", w2.at[:, rows], w2c.at[h, v_there, :, :, left], yn)
        add(f"fQ{h}", w2c.at[h, v_here, :, :, left], w2c.at[h, v_here, :, :, right], sib)
    o_base = len(copies)

    def out_copies(t):
        rows = pl.ds(pl.multiple_of(t * TT, TT), TT)
        there = pl.ds(pl.multiple_of(c * tok + t * TT, TT), TT)
        return [pltpu.make_async_remote_copy(
            src_ref=hn.at[j, rows], dst_ref=y_out.at[there, pl.ds(j * W, W)],
            send_sem=send.at[o_base + 3 * t + j], recv_sem=recv.at[o_base + 3 * t + j],
            device_id=sib, device_id_type=MESH) for j in range(3)]

    def serve(name):
        got(name)
        start("f" + name)
        start(*NEXT.get(name, ()))

    def w1_loads(i):
        kind, far, k = STEPS[i][:3]
        slot = i % 2
        part = pl.ds(k * W, W)
        if far:
            srcs = (wx_o.at[k], wd_o.at[k], wx_s.at[k], wd_s.at[k])
        else:
            srcs = (w1.at[:, part], wy_o.at[k], ws.at[:, part], wy_s.at[k])
        out = []
        for j, s in enumerate(srcs):
            rows = at(y if j % 2 == 0 else 1 - y, dh)
            who = c if j < 2 else 1 - c
            if kind == "full":
                out.append((s, w1b.at[slot, rows, at(who, W)], lsem.at[slot, j]))
            elif kind == "hid" or j % 2 == 0:
                for b in range(2):
                    lanes = pl.ds(pl.multiple_of(b * W + who * HW, 128), HW)
                    out.append((s.at[:, pl.ds(b * HW, HW)], w1b.at[slot, rows, lanes], lsem.at[slot, 2 * j + b]))
        return out

    def w2_loads(i, own, oth):
        _, far, k = STEPS[i][:3]
        slot, part = i % 2, pl.ds(k * W, W)
        return [(own.at[:, part], w2b.at[slot, :, :, pl.ds(0, cols)], lsem.at[slot, 8]),
                (oth.at[:, part], w2b.at[slot, :, :, pl.ds(cols, cols)], lsem.at[slot, 9])]

    waited = set()

    def begin(many):
        for d in many:
            pltpu.make_async_copy(*d).start()

    def load(i):
        kind, far, k = STEPS[i][:3]
        if kind in ("comp", "last", "own"):
            return
        need = [f"fD{k}" if far else f"fY{k}"]
        if kind == "full":
            need += [f"fV{k}"] + ([f"fB{k}" if k < 4 else f"fA{k}"] if far else [])
        got(*(n for n in need if n not in waited))
        waited.update(need)
        begin(w1_loads(i))
        if kind == "full":
            local = jnp.logical_not(same) if far else same

            @pl.when(local)
            def _():
                begin(w2_loads(i, w2, w2s))

            @pl.when(jnp.logical_not(local))
            def _():
                begin(w2_loads(i, w2y_o, w2y_s))

    def loaded(i):
        kind, _, k = STEPS[i][:3]
        if kind in ("comp", "last"):
            got(f"fP{k}", f"fQ{k}")
        if kind in ("comp", "last", "own"):
            return
        for d in w1_loads(i) + (w2_loads(i, w2, w2s) if kind == "full" else []):
            pltpu.make_async_copy(*d).wait()

    barrier = pltpu.get_barrier_semaphore()
    for dev in (sib, xn, xn2, yn):
        pl.semaphore_signal(barrier, inc=1, device_id=dev, device_id_type=MESH)
    pl.semaphore_wait(barrier, 4)

    first = NEXT[None]
    start(*first[:1], "Xc", "ws", "w2s", *first[1:])
    own = pltpu.make_async_copy(x_in.at[my_tok], xs.at[:, my_cols], osem)
    own.start()

    keep = []
    for h in range(4):
        rows = pl.ds((6 + h // 2) * W + (h % 2) * HW, HW)
        for j, src in enumerate((w2, w2s)):
            keep.append((src.at[:, rows], w2c.at[h, v_there, :, :, pl.ds(j * cols, cols)], csem.at[h, j]))
    begin(keep[::2])

    @pl.loop(0, nt)
    def _(t):
        acc[pl.ds(t * TT, TT), :] = jnp.zeros((TT, acc.shape[1]), jnp.float32)

    got("ws", "w2s")
    begin(keep[1::2])
    for d in keep:
        pltpu.make_async_copy(*d).wait()
    own.wait()
    got("Xc")

    n_steps = len(STEPS)
    f32 = jnp.float32

    def before(b):
        i, t = TILES[b]
        for name in HOOKS.get(b, ()):
            if name[0] == "L":
                load(int(name[1:]))
            else:
                serve(name)
        if b in FIRST:
            loaded(i)
        if b in NEW_X:
            got(f"Xx{t}", f"Xz{t}")

    @pl.loop(0, N_TILES)
    def _(b):
        def pick(lo, hi):
            if not any(n in busy for n in range(lo, hi)):
                return lambda: None
            if hi - lo == 1:
                return functools.partial(before, lo)
            mid = (lo + hi) // 2
            low, high = pick(lo, mid), pick(mid, hi)
            return lambda: lax.cond(b < mid, low, high)

        busy = set(HOOKS) | set(FIRST) | set(NEW_X)
        pick(0, N_TILES)()

        i, t = step_and_tile(b)
        slot = lax.rem(i, 2)
        rows = at(t, TT, TT)

        subs = [pl.ds(pl.multiple_of(t * TT + q * ST, ST), ST) for q in range(TT // ST)]

        @pl.when(is_kind(i, ("full",)))
        def _():
            ps = [jnp.dot(xs[r, :], w1b[slot], preferred_element_type=f32) for r in subs]
            for r, p in zip(subs, ps):
                h = gelu(p).astype(BF)
                v = w2b[slot].reshape(2 * W, 2 * cols)
                acc[r, :] += jnp.dot(h, v, preferred_element_type=f32)

        @pl.when(is_kind(i, ("hid",)))
        def _():
            k2 = 2 * is_kind(i, ("hid", 0, 7)).astype(jnp.int32)
            ps = [jnp.dot(xs[r, :], w1b[slot], preferred_element_type=f32) for r in subs]
            for r, p in zip(subs, ps):
                h = gelu(p).astype(BF)
                hn[k2, r, :] = h[:, :W]
                hn[k2 + 1, r, :] = h[:, W:]

        @pl.when(is_kind(i, ("part",)))
        def _():
            k2 = 2 * is_kind(i, ("part", 1, 7)).astype(jnp.int32)
            p = jnp.dot(xs[rows, at(y, dh)], w1b[slot, at(y, dh), :], preferred_element_type=f32)
            p32[k2, rows, :] = p[:, :W]
            p32[k2 + 1, rows, :] = p[:, W:]

        def far_p(j):
            return [p32[j, r, :] + jnp.dot(xs[r, at(1 - y, dh)], wl[j], preferred_element_type=f32) for r in subs]

        def down(j, half, lo, hi):
            return w2c[j, half, :, :, lo * cols:hi * cols].reshape(2 * HW, (hi - lo) * cols)

        @pl.when(is_kind(i, ("comp",)))
        def _():
            j = i - STEPS.index(("comp", 1, 0, 0, NT))
            for r, p in zip(subs, far_p(j)):
                total = acc[r, :] + jnp.dot(hn[j, r, :], down(j, 0, 0, 2), preferred_element_type=f32)
                acc[r, :] = total + jnp.dot(gelu(p).astype(BF), down(j, 1, 0, 2), preferred_element_type=f32)

        @pl.when(is_kind(i, ("last",)))
        def _():
            for r, p in zip(subs, far_p(3)):
                h = gelu(p).astype(BF)
                w1b[0, r, :W] = h
                total = acc[r, cols:] + jnp.dot(hn[3, r, :], down(3, 0, 1, 2), preferred_element_type=f32)
                total = (total + jnp.dot(h, down(3, 1, 1, 2), preferred_element_type=f32)).astype(BF)
                for m in range(3):
                    hn[m, r, :] = total[:, m * W:(m + 1) * W]

            @pl.when(t > 0)
            def _():
                for d in out_copies(t - 1):
                    d.start()

        @pl.when(is_kind(i, ("own",)))
        def _():
            @pl.when(t == 0)
            def _():
                for d in out_copies(nt - 1):
                    d.start()

            h = jnp.concatenate([hn[3, rows, :], w1b[0, rows, :W]], axis=1)
            total = acc[rows, :cols] + jnp.dot(h, w2c[3, :, :, :, :cols].reshape(4 * HW, cols), preferred_element_type=f32)
            y_out[pl.ds(pl.multiple_of(c * tok + t * TT, TT), TT), :] = total.astype(BF)

    for cp in copies.values():
        cp().wait_send()
    for t in range(nt):
        for d in out_copies(t):
            d.wait()


def solution(mesh):
    def local_mlp(x_blk, w1, w2):
        rows, cols = x_blk.shape
        dh, fq = w1.shape
        tok = rows // 2
        nk = fq // W
        w2v = w2.reshape(2, fq, cols)
        land = jax.ShapeDtypeStruct((nk, dh, W), BF)
        down = jax.ShapeDtypeStruct(w2v.shape, BF)
        n_copies = 3 + 2 * NT + 4 * nk + 4 * 6 + 16 + 3 * NT
        dma = pltpu.SemaphoreType.DMA
        outs = pl.pallas_call(
            kernel,
            out_shape=[pltpu.VMEM(x_blk.shape, BF), jax.ShapeDtypeStruct(w1.shape, BF)] + [land] * 6 + [down] * 3,
            in_specs=[pl.BlockSpec(memory_space=pl.ANY)] * 3,
            out_specs=[pl.BlockSpec(memory_space=pltpu.VMEM)] + [pl.BlockSpec(memory_space=pl.ANY)] * 10,
            scratch_shapes=[
                pltpu.VMEM((tok, 4 * cols), BF),
                pltpu.VMEM((tok, 2 * cols), jnp.float32),
                pltpu.VMEM((2, 2 * dh, 2 * W), BF),
                pltpu.VMEM((2, 2, W, 2 * cols), BF),
                pltpu.VMEM((4, tok, W), jnp.float32),
                pltpu.VMEM((4, tok, W), BF),
                pltpu.VMEM((4, dh, W), BF),
                pltpu.VMEM((4, 2, 2, HW, 2 * cols), BF),
                dma((n_copies,)), dma((n_copies,)), dma((2, 10)), dma, dma((4, 2)),
            ],
            compiler_params=pltpu.CompilerParams(
                collective_id=0, has_side_effects=True, vmem_limit_bytes=60_700_000),
        )(x_blk, w1, w2v)
        return outs[0]

    act_spec = P(ROW_AXES, COL_AXES)
    wgt_spec = P("row", COL_AXES)
    return jax.shard_map(local_mlp, mesh=mesh, in_specs=(act_spec, wgt_spec, wgt_spec), out_specs=act_spec, check_vma=False)
```

```python
import functools

import jax
import jax.numpy as jnp
from jax import lax
from jax.experimental import pallas as pl
from jax.experimental.pallas import tpu as pltpu
from jax.sharding import PartitionSpec as P

ROW_AXES = ("dp", "row")
COL_AXES = ("co", "ci")
MESH = pl.DeviceIdType.MESH
BF = jnp.bfloat16
GELU_A = 0.7978845608028654

W = 256
HW = W // 2
TT = 512
ST = TT // 2

STEPS = (
    ("hid", 0, 6, 0, 3), ("hid", 0, 7, 0, 3), ("full", 0, 1, 0, 4), ("full", 0, 5, 0, 3),
    ("hid", 0, 7, 3, 4), ("full", 0, 3, 0, 4), ("full", 0, 5, 3, 4), ("full", 0, 4, 1, 4),
    ("hid", 0, 6, 3, 4), ("full", 0, 4, 0, 1), ("full", 1, 5, 0, 4), ("full", 0, 0, 0, 4),
    ("full", 1, 4, 2, 4), ("full", 1, 4, 0, 1), ("full", 0, 2, 0, 4), ("full", 1, 3, 0, 4),
    ("full", 1, 4, 1, 2), ("full", 1, 2, 0, 4), ("full", 1, 0, 0, 4), ("part", 1, 6, 0, 4),
    ("full", 1, 1, 0, 4), ("part", 1, 7, 0, 4), ("six", 1, 6, 0, 4), ("comp", 1, 2, 0, 4),
    ("last", 1, 3, 0, 4), ("own", 1, 3, 0, 4),
)
LINK_X = (
    "Xx1", "Xx2", "Xz0", "Xz2", "Xz1", "Xx0", "Xz3", "D5", "Xx3", "A5", "D4", "D3",
    "A4", "D2", "D0", "D1", "D6", "P0", "D7", "P1", "P2", "P3",
)
LINK_Y = (
    "Y6", "V3", "V1", "Y1", "Y5", "Y7", "V5", "Y3", "Y4", "V4", "V0", "Y0",
    "V2", "Y2", "B3", "B2", "B0", "B1", "Q0", "Q1", "Q2", "Q3",
)
HOOKS = {
    0: ("Y7", "Y6", "V1", "Y1", "L0",),
    1: ("Y5",),
    2: ("L1",),
    3: ("L2",),
    6: ("V5",),
    7: ("L3",),
    8: ("Y3",),
    10: ("Y4",),
    12: ("V3", "L4",),
    13: ("L5",),
    14: ("D5",),
    15: ("L6",),
    16: ("V4",),
    18: ("L7",),
    19: ("A5",),
    21: ("V0", "L8",),
    22: ("Y0", "D4", "L9",),
    23: ("L10",),
    27: ("D3", "L11",),
    28: ("V2", "A4",),
    30: ("L12",),
    32: ("L13",),
    33: ("D2",),
    34: ("Y2", "L14",),
    38: ("B3", "L15",),
    40: ("L16",),
    41: ("D0",),
    42: ("B2",),
    43: ("L17",),
    44: ("D1",),
    47: ("B0", "D6", "L18",),
    51: ("L19",),
    52: ("B1",),
    53: ("P0",),
    54: ("L20",),
    58: ("D7",),
    59: ("L21",),
    60: ("Q0",),
    61: ("Q1", "P1"),
    67: ("Q2", "P2"),
    70: ("P3", "Q3"),
}
NT = 4
TILES = [(i, t) for i, s in enumerate(STEPS) for t in range(s[3], s[4])]
N_TILES = len(TILES)
FIRST = [TILES.index((i, s[3])) for i, s in enumerate(STEPS)]
NEW_X = [min(b for b in range(N_TILES) if TILES[b][1] == t) for t in range(NT)]


def links_after():
    def wants(n):
        k = int(n[-1])
        return {"A": f"Y{k}", "B": f"D{k}", "P": f"Y{6 + k // 2}"}.get(n[0])

    served, at, res = set(), [0, 0], {}
    events = [None] + [n for b in sorted(HOOKS) for n in HOOKS[b] if n[0] != "L"]
    for e in events:
        served.add(e)
        new = []
        for j, link in enumerate((LINK_X, LINK_Y)):
            while at[j] < len(link) and (wants(link[at[j]]) is None or wants(link[at[j]]) in served):
                new.append(link[at[j]])
                at[j] += 1
        res[e] = tuple(new)
    assert at == [len(LINK_X), len(LINK_Y)]
    return res


NEXT = links_after()


def is_kind(i, kind):
    mask = sum(1 << n for n, s in enumerate(STEPS) if s[:len(kind)] == kind)
    return lax.rem(lax.shift_right_logical(jnp.int32(mask), i), 2) == 1


def gelu(p):
    u = p * (GELU_A + (GELU_A * 0.044715) * (p * p))
    return (0.5 * p) * (1.0 + jnp.tanh(u))


def kernel(x_in, w1, w2, y_out, ws, wy_o, wy_s, wx_o, wx_s, wd_o, wd_s, w2s, w2y_o, w2y_s,
           xs, acc, w1b, w2b, p32, hn, wl, w2c, send, recv, lsem, osem, csem):
    dp, y, x, c = (lax.axis_index(a) for a in ("dp", "row", "co", "ci"))
    tok = x_in.shape[0] // 2
    dh = w1.shape[0]
    cols = x_in.shape[1]
    nk = w1.shape[1] // W
    nt = NT
    assert tok == NT * TT and nk == 8
    sib, xn, yn = (dp, y, x, 1 - c), (dp, y, 1 - x, c), (dp, 1 - y, x, c)
    xn2 = (dp, y, 1 - x, 1 - c)
    same = x == y
    v_here = jnp.where(same, 1, 0)
    v_there = 1 - v_here

    copies = {}

    def add(name, src, dst, dev):
        i = len(copies)
        copies[name] = functools.partial(
            pltpu.make_async_remote_copy,
            src_ref=src, dst_ref=dst, send_sem=send.at[i], recv_sem=recv.at[i],
            device_id=dev, device_id_type=MESH)

    def start(*names):
        for n in names:
            copies[n]().start()

    def got(*names):
        for n in names:
            copies[n]().wait_recv()

    def at(i, n, unit=128):
        return pl.ds(pl.multiple_of(i * n, unit), n)

    my_cols = at(x * 2 + c, cols)
    my_tok, sib_tok = at(c, tok), at(1 - c, tok)
    add("Xc", x_in.at[sib_tok], xs.at[:, my_cols], sib)
    for q in range(NT):
        for name, who, dev in (("Xx", c, xn), ("Xz", 1 - c, xn2)):
            src = x_in.at[pl.ds(pl.multiple_of(who * tok + q * TT, TT), TT)]
            add(f"{name}{q}", src, xs.at[pl.ds(q * TT, TT), my_cols], dev)
    add("ws", w1, ws, sib)
    add("w2s", w2, w2s, sib)
    for k in range(nk):
        part = pl.ds(k * W, W)
        add(f"Y{k}", w1.at[:, part], wy_o.at[k], yn)
        add(f"fY{k}", wy_o.at[k], wy_s.at[k], sib)
        add(f"D{k}", w1.at[:, part], wx_o.at[k], xn)
        add(f"fD{k}", wx_o.at[k], wx_s.at[k], sib)
        if k < 6:
            add(f"V{k}", w2.at[:, part], w2y_o.at[:, part], yn)
            add(f"fV{k}", w2y_o.at[:, part], w2y_s.at[:, part], sib)
            way = ("B", wx_o, yn) if k < 4 else ("A", wy_o, xn)
            add(f"{way[0]}{k}", way[1].at[k], wd_o.at[k], way[2])
            add(f"f{way[0]}{k}", wd_o.at[k], wd_s.at[k], sib)
    for h in range(4):
        k, half = 6 + h // 2, pl.ds((h % 2) * HW, HW)
        rows = pl.ds(k * W + (h % 2) * HW, HW)
        mine = wl.at[h, :, at(c, HW)]
        add(f"P{h}", wy_o.at[k, :, half], mine, xn)
        add(f"fP{h}", mine, mine, sib)
        left, right = pl.ds(0, cols), pl.ds(cols, cols)
        add(f"Q{h}", w2.at[:, rows], w2c.at[h, v_there, :, :, left], yn)
        add(f"fQ{h}", w2c.at[h, v_here, :, :, left], w2c.at[h, v_here, :, :, right], sib)
    o_base = len(copies)

    def out_copies(t):
        rows = pl.ds(pl.multiple_of(t * TT, TT), TT)
        there = pl.ds(pl.multiple_of(c * tok + t * TT, TT), TT)
        return [pltpu.make_async_remote_copy(
            src_ref=hn.at[j, rows], dst_ref=y_out.at[there, pl.ds(j * W, W)],
            send_sem=send.at[o_base + 3 * t + j], recv_sem=recv.at[o_base + 3 * t + j],
            device_id=sib, device_id_type=MESH) for j in range(3)]

    def serve(name):
        got(name)
        start("f" + name)
        start(*NEXT.get(name, ()))

    def w1_loads(i):
        kind, far, k = STEPS[i][:3]
        slot = i % 2
        part = pl.ds(k * W, W)
        if far:
            srcs = (wx_o.at[k], wd_o.at[k], wx_s.at[k], wd_s.at[k])
        else:
            srcs = (w1.at[:, part], wy_o.at[k], ws.at[:, part], wy_s.at[k])
        out = []
        for j, s in enumerate(srcs):
            rows = at(y if j % 2 == 0 else 1 - y, dh)
            who = c if j < 2 else 1 - c
            if kind == "full":
                out.append((s, w1b.at[slot, rows, at(who, W)], lsem.at[slot, j]))
            elif kind == "hid" or j % 2 == 0:
                for b in range(2):
                    lanes = pl.ds(pl.multiple_of(b * W + who * HW, 128), HW)
                    out.append((s.at[:, pl.ds(b * HW, HW)], w1b.at[slot, rows, lanes], lsem.at[slot, 2 * j + b]))
        return out

    def w2_loads(i, own, oth):
        _, far, k = STEPS[i][:3]
        slot, part = i % 2, pl.ds(k * W, W)
        return [(own.at[:, part], w2b.at[slot, :, :, pl.ds(0, cols)], lsem.at[slot, 8]),
                (oth.at[:, part], w2b.at[slot, :, :, pl.ds(cols, cols)], lsem.at[slot, 9])]

    waited = set()

    def begin(many):
        for d in many:
            pltpu.make_async_copy(*d).start()

    def load(i):
        kind, far, k = STEPS[i][:3]
        if kind in ("six", "comp", "last", "own"):
            return
        need = [f"fD{k}" if far else f"fY{k}"]
        if kind == "full":
            need += [f"fV{k}"] + ([f"fB{k}" if k < 4 else f"fA{k}"] if far else [])
        got(*(n for n in need if n not in waited))
        waited.update(need)
        begin(w1_loads(i))
        if kind == "full":
            local = jnp.logical_not(same) if far else same

            @pl.when(local)
            def _():
                begin(w2_loads(i, w2, w2s))

            @pl.when(jnp.logical_not(local))
            def _():
                begin(w2_loads(i, w2y_o, w2y_s))

    def loaded(i):
        kind, _, k = STEPS[i][:3]
        if kind in ("comp", "last"):
            got(f"fP{k}", f"fQ{k}")
        if kind == "six":
            got("fP0", "fQ0", "fP1", "fQ1")
        if kind in ("six", "comp", "last", "own"):
            return
        for d in w1_loads(i) + (w2_loads(i, w2, w2s) if kind == "full" else []):
            pltpu.make_async_copy(*d).wait()

    barrier = pltpu.get_barrier_semaphore()
    for dev in (sib, xn, xn2, yn):
        pl.semaphore_signal(barrier, inc=1, device_id=dev, device_id_type=MESH)
    pl.semaphore_wait(barrier, 4)

    first = NEXT[None]
    start(*first[:1], "Xc", "ws", "w2s", *first[1:])
    own = pltpu.make_async_copy(x_in.at[my_tok], xs.at[:, my_cols], osem)
    own.start()

    keep = []
    for h in range(4):
        rows = pl.ds((6 + h // 2) * W + (h % 2) * HW, HW)
        for j, src in enumerate((w2, w2s)):
            keep.append((src.at[:, rows], w2c.at[h, v_there, :, :, pl.ds(j * cols, cols)], csem.at[h, j]))
    begin(keep[::2])

    @pl.loop(0, nt)
    def _(t):
        acc[pl.ds(t * TT, TT), :] = jnp.zeros((TT, acc.shape[1]), jnp.float32)

    got("ws", "w2s")
    begin(keep[1::2])
    for d in keep:
        pltpu.make_async_copy(*d).wait()
    own.wait()
    got("Xc")

    n_steps = len(STEPS)
    f32 = jnp.float32

    def before(b):
        i, t = TILES[b]
        for name in HOOKS.get(b, ()):
            if name[0] == "L":
                load(int(name[1:]))
            else:
                serve(name)
        if b in FIRST:
            loaded(i)
        if b in NEW_X:
            got(f"Xx{t}", f"Xz{t}")

    @pl.loop(0, N_TILES)
    def _(b):
        def pick(lo, hi):
            if hi - lo == 1:
                def leaf():
                    if lo in busy:
                        before(lo)
                    return tuple(jnp.int32(v) for v in TILES[lo])
                return leaf
            mid = (lo + hi) // 2
            low, high = pick(lo, mid), pick(mid, hi)
            return lambda: lax.cond(b < mid, low, high)

        busy = set(HOOKS) | set(FIRST) | set(NEW_X)
        i, t = pick(0, N_TILES)()
        slot = lax.rem(i, 2)
        rows = at(t, TT, TT)

        subs = [pl.ds(pl.multiple_of(t * TT + q * ST, ST), ST) for q in range(TT // ST)]

        @pl.when(is_kind(i, ("full",)))
        def _():
            ps = [jnp.dot(xs[r, :], w1b[slot], preferred_element_type=f32) for r in subs]
            for r, p in zip(subs, ps):
                h = gelu(p).astype(BF)
                v = w2b[slot].reshape(2 * W, 2 * cols)
                acc[r, :] += jnp.dot(h, v, preferred_element_type=f32)

        @pl.when(is_kind(i, ("hid",)))
        def _():
            k2 = 2 * is_kind(i, ("hid", 0, 7)).astype(jnp.int32)
            ps = [jnp.dot(xs[r, :], w1b[slot], preferred_element_type=f32) for r in subs]
            for r, p in zip(subs, ps):
                h = gelu(p).astype(BF)
                hn[k2, r, :] = h[:, :W]
                hn[k2 + 1, r, :] = h[:, W:]

        @pl.when(is_kind(i, ("part",)))
        def _():
            k2 = 2 * is_kind(i, ("part", 1, 7)).astype(jnp.int32)
            p = jnp.dot(xs[rows, at(y, dh)], w1b[slot, at(y, dh), :], preferred_element_type=f32)
            p32[k2, rows, :] = p[:, :W]
            p32[k2 + 1, rows, :] = p[:, W:]

        def far_p(j):
            return [p32[j, r, :] + jnp.dot(xs[r, at(1 - y, dh)], wl[j], preferred_element_type=f32) for r in subs]

        def down(j, half, lo, hi):
            return w2c[j, half, :, :, lo * cols:hi * cols].reshape(2 * HW, (hi - lo) * cols)

        @pl.when(is_kind(i, ("six",)))
        def _():
            both = range(2)
            ps = [jnp.dot(xs[r, at(1 - y, dh)], jnp.concatenate([wl[j] for j in both], axis=1), preferred_element_type=f32)
                  for r in subs]
            for r, p in zip(subs, ps):
                hs = []
                for j in both:
                    hs += [hn[j, r, :], gelu(p32[j, r, :] + p[:, j * W:(j + 1) * W]).astype(BF)]
                v = w2c[0:2].reshape(8 * HW, 2 * cols)
                acc[r, :] += jnp.dot(jnp.concatenate(hs, axis=1), v, preferred_element_type=f32)

        @pl.when(is_kind(i, ("comp",)))
        def _():
            j = 2
            for r, p in zip(subs, far_p(j)):
                total = acc[r, :] + jnp.dot(hn[j, r, :], down(j, 0, 0, 2), preferred_element_type=f32)
                acc[r, :] = total + jnp.dot(gelu(p).astype(BF), down(j, 1, 0, 2), preferred_element_type=f32)

        @pl.when(is_kind(i, ("last",)))
        def _():
            for r, p in zip(subs, far_p(3)):
                h = gelu(p).astype(BF)
                w1b[0, r, :W] = h
                total = acc[r, cols:] + jnp.dot(hn[3, r, :], down(3, 0, 1, 2), preferred_element_type=f32)
                total = (total + jnp.dot(h, down(3, 1, 1, 2), preferred_element_type=f32)).astype(BF)
                for m in range(3):
                    hn[m, r, :] = total[:, m * W:(m + 1) * W]

            @pl.when(t > 0)
            def _():
                for d in out_copies(t - 1):
                    d.start()

        @pl.when(is_kind(i, ("own",)))
        def _():
            @pl.when(t == 0)
            def _():
                for d in out_copies(nt - 1):
                    d.start()

            h = jnp.concatenate([hn[3, rows, :], w1b[0, rows, :W]], axis=1)
            total = acc[rows, :cols] + jnp.dot(h, w2c[3, :, :, :, :cols].reshape(4 * HW, cols), preferred_element_type=f32)
            y_out[pl.ds(pl.multiple_of(c * tok + t * TT, TT), TT), :] = total.astype(BF)

    for cp in copies.values():
        cp().wait_send()
    for t in range(nt):
        for d in out_copies(t):
            d.wait()


def solution(mesh):
    def local_mlp(x_blk, w1, w2):
        rows, cols = x_blk.shape
        dh, fq = w1.shape
        tok = rows // 2
        nk = fq // W
        w2v = w2.reshape(2, fq, cols)
        land = jax.ShapeDtypeStruct((nk, dh, W), BF)
        down = jax.ShapeDtypeStruct(w2v.shape, BF)
        n_copies = 3 + 2 * NT + 4 * nk + 4 * 6 + 16 + 3 * NT
        dma = pltpu.SemaphoreType.DMA
        outs = pl.pallas_call(
            kernel,
            out_shape=[pltpu.VMEM(x_blk.shape, BF), jax.ShapeDtypeStruct(w1.shape, BF)] + [land] * 6 + [down] * 3,
            in_specs=[pl.BlockSpec(memory_space=pl.ANY)] * 3,
            out_specs=[pl.BlockSpec(memory_space=pltpu.VMEM)] + [pl.BlockSpec(memory_space=pl.ANY)] * 10,
            scratch_shapes=[
                pltpu.VMEM((tok, 4 * cols), BF),
                pltpu.VMEM((tok, 2 * cols), jnp.float32),
                pltpu.VMEM((2, 2 * dh, 2 * W), BF),
                pltpu.VMEM((2, 2, W, 2 * cols), BF),
                pltpu.VMEM((4, tok, W), jnp.float32),
                pltpu.VMEM((4, tok, W), BF),
                pltpu.VMEM((4, dh, W), BF),
                pltpu.VMEM((4, 2, 2, HW, 2 * cols), BF),
                dma((n_copies,)), dma((n_copies,)), dma((2, 10)), dma, dma((4, 2)),
            ],
            compiler_params=pltpu.CompilerParams(
                collective_id=0, has_side_effects=True, vmem_limit_bytes=60_700_000),
        )(x_blk, w1, w2v)
        return outs[0]

    act_spec = P(ROW_AXES, COL_AXES)
    wgt_spec = P("row", COL_AXES)
    return jax.shard_map(local_mlp, mesh=mesh, in_specs=(act_spec, wgt_spec, wgt_spec), out_specs=act_spec, check_vma=False)
```
